32 devices in a mesh: row: 8 (over y, x, core), col: 4 (over z).
Axes of the slice: x: 2, y: 2, z: 4, core: 2. Of those that a mesh axis runs over, the one named last changes fastest.
Arguments:
- row_cells: int32 [3, 8192], P(None, 'row'), may hold values from 0 to 63
- col_cells: int32 [3, 32768], P(None, 'col'), may hold values from 0 to 63
- omega: float32 [16, 32768], P(None, 'col'), may hold values from -6 to 6
Outputs:
- basis: float32 [16, 8192], P(None, 'row')
- image: float32 [16, 32768], P(None, 'col')
- core: float32 [16, 16], replicated
The draws below stay inside these ranges and needn't reach their ends.
All inputs are finite; a program needn't handle non-finite values.
Results may differ from the reference program's by a relative error of at most 0.0001.
Values sent between devices are 32-bit elements; how exact they have to be, the bound alone decides.
A program may use at most 64 MiB of HBM per device.

```python
import math
import jax
import jax.numpy as jnp
from jax import lax

RANK = 16
GRID = 64
ROWS = 8192
ORDER = 32768


def plant(array, rng, least, top_value):
    index_at = [jax.random.randint(jax.random.fold_in(rng, axis), (), 0, length) for axis, length in enumerate(array.shape)]
    longest = array.shape.index(max(array.shape))
    neighbour = index_at[:longest] + [(index_at[longest] + 1) % array.shape[longest]] + index_at[longest + 1:]
    return array.at[tuple(index_at)].set(least).at[tuple(neighbour)].set(top_value)


def level_of(key, extent, cuts, low, high):
    level, own = 1.0, jax.random.fold_in(key, 6)
    for position, blocks in cuts:
        draws = jnp.exp(jax.random.uniform(jax.random.fold_in(own, position), (blocks,), jnp.float32, low / len(cuts), high / len(cuts)))
        level = level * jnp.repeat(draws, extent[position] // blocks).reshape([-1 if axis == position else 1 for axis in range(len(extent))])
    return level


def noise(stream_key, extent, deviation, limit, cuts=(), dtype=jnp.bfloat16):
    factor_of = level_of(stream_key, extent, cuts, -0.22, 0.18) if cuts else 1.0
    values = jax.random.normal(stream_key, extent, jnp.float32) * deviation * factor_of
    return jnp.minimum(jnp.maximum(values, -limit), limit).astype(dtype)


def setup_inputs(seed: int = 0) -> dict:
    splits = jax.random.split(jax.random.key(seed), 4)
    return {
        "row_cells": plant(jax.random.randint(splits[0], (3, ROWS), 0, GRID), jax.random.fold_in(splits[0], 1), 0, GRID - 1).astype(jnp.int32),
        "col_cells": plant(jax.random.randint(splits[1], (3, ORDER), 0, GRID), jax.random.fold_in(splits[1], 1), 0, GRID - 1).astype(jnp.int32),
        "omega": noise(splits[2], (RANK, ORDER), 1.0, 6.0, ((1, 4),), jnp.float32),
    }


def kernel_tile(rows, cols):
    first = (rows[0][:, None] - cols[0][None, :]).astype(jnp.float32)
    total = first * first
    second = (rows[1][:, None] - cols[1][None, :]).astype(jnp.float32)
    total = total + second * second
    third = (rows[2][:, None] - cols[2][None, :]).astype(jnp.float32)
    total = total + third * third
    return 0.25 * jnp.exp(-jnp.sqrt(total) / 6.4)

def reference(row_cells, col_cells, omega):
    rows_total = row_cells.shape[1]
    order = col_cells.shape[1]
    rank = omega.shape[0]
    block = math.gcd(rows_total, 512)
    count = rows_total // block
    row_blocks = row_cells.reshape(3, count, block).transpose(1, 0, 2)

    def sketch_block(cells):
        tile = kernel_tile(cells, col_cells)
        return lax.dot_general(omega, tile, (((1,), (1,)), ((), ())), precision=lax.Precision.HIGHEST)
    parts = lax.map(sketch_block, row_blocks)
    sketch = parts.transpose(1, 0, 2).reshape(rank, rows_total)
    gram = jnp.dot(sketch, sketch.T, precision=lax.Precision.HIGHEST) / rows_total
    lower = jnp.linalg.cholesky(gram)
    basis = jax.scipy.linalg.solve_triangular(lower, sketch, lower=True)
    basis_blocks = basis.reshape(rank, count, block).transpose(1, 0, 2)

    def image_step(carry, pair):
        cells, left = pair
        tile = kernel_tile(cells, col_cells)
        return (carry + jnp.dot(left, tile, precision=lax.Precision.HIGHEST), None)
    image, _ = lax.scan(image_step, jnp.zeros((rank, order), jnp.float32), (row_blocks, basis_blocks))
    core = jnp.dot(image, image.T, precision=lax.Precision.HIGHEST) / order
    return (basis, image, core)
```

```python
import functools
import math

import jax
import jax.numpy as jnp
from jax import lax
from jax.experimental import pallas as pl
from jax.experimental.pallas import tpu as pltpu
from jax.sharding import PartitionSpec as P

BF16, F32 = jnp.bfloat16, jnp.float32
HIGHEST = lax.Precision.HIGHEST
NT = (((1,), (1,)), ((), ()))
NN = (((1,), (0,)), ((), ()))
LANES = 128
RATE = -math.log2(math.e) / 6.4
UNIT = 256
LEAD = 3
BUFS = 4
SLICE = 64


def split(x):
    high = x.astype(BF16)
    return high, (x - high.astype(F32)).astype(BF16)


def features(cells, left):
    x = [cells[d : d + 1, :].astype(F32) - 32.0 for d in range(3)]
    norm = x[0] * x[0] + x[1] * x[1] + x[2] * x[2]
    high = jnp.floor(norm * 0.0625) * 16.0
    low = norm - high
    one, zero = jnp.ones_like(norm), jnp.zeros_like(norm)
    if left:
        rows = [-2.0 * x[0], -2.0 * x[1], -2.0 * x[2], one, one, high, low, zero]
    else:
        rows = [x[0], x[1], x[2], high, low, one, one, zero]
    return jnp.concatenate(rows, axis=0)


def kernel(
    shape,
    row_hbm, col_hbm, omega_hbm,
    basis_ref, image_ref, core_ref,
    row_in, col_in, om_in, rowf, colf, om, khi, klo, sq0, sq1, sq2, sq3, hi0, hi1, lo0, lo1,
    sk_src, sk_all, sk_hl, g_src, g_all, wp, s_in, w_src, w_all, img, c_src, c_all, d_src, d_all,
    in_s, sk_ss, sk_rs, g_ss, g_rs, p_ss, p_rs, w_ss, w_rs, a_ss, a_rs, f_ss, f_rs, c_ss, c_rs, d_ss, d_rs,
):
    R, C, rank, M, N, rows_total, order = shape
    me = lax.axis_index("row")
    mc = lax.axis_index("col")
    half = R // 2
    side = lax.rem(me, 2)
    chip = me // 2
    sib = me + 1 - 2 * side
    part = N // R
    chunk = min(M, UNIT)
    chunks = M // chunk
    units = N // UNIT
    sq = (sq0, sq1, sq2, sq3)
    hi, lo = (hi0, hi1), (lo0, lo1)
    binary = half & (half - 1) == 0
    far_first = sorted(range(1, half), key=lambda t: -bin(t).count("1"))

    def row_of(t):
        return lax.rem(me + t, R)

    def chip_to(t):
        if not binary:
            return lax.rem(chip + t, half)
        total, bit = 0, 1
        while bit < half:
            total = total + bit * lax.rem(chip // bit + t // bit, 2)
            bit *= 2
        return total

    def chip_from(t):
        return chip_to(t) if binary else lax.rem(chip + half - t, half)

    def remote(src, dst, ss, rs, axis, peer):
        return pltpu.make_async_remote_copy(
            src_ref=src, dst_ref=dst, send_sem=ss, recv_sem=rs,
            device_id={axis: peer}, device_id_type=pl.DeviceIdType.MESH,
        )

    loads = [
        pltpu.make_async_copy(source, target, in_s.at[i])
        for i, (source, target) in enumerate(((col_hbm, col_in), (row_hbm, row_in), (omega_hbm, om_in)))
    ]
    for load in loads:
        load.start()
    barrier = pltpu.get_barrier_semaphore()
    for t in range(1, R):
        pl.semaphore_signal(barrier, inc=1, device_id={"row": row_of(t)}, device_id_type=pl.DeviceIdType.MESH)
    for t in range(1, C):
        pl.semaphore_signal(
            barrier, inc=1, device_id={"col": lax.rem(mc + t, C)}, device_id_type=pl.DeviceIdType.MESH
        )

    loads[0].wait()
    loads[1].wait()
    rowf[0:8, :] = features(row_in[...], False).astype(BF16)
    rowf[8:16, :] = jnp.zeros((8, M), BF16)
    step = min(N, 1024)
    for s in range(N // step):
        left = features(col_in[:, s * step : (s + 1) * step], True)
        for b in range(step // LANES):
            block = jnp.concatenate(
                [left[:, b * LANES : (b + 1) * LANES], jnp.zeros((LANES - 8, LANES), F32)], axis=0
            )
            colf[s * step + b * LANES : s * step + (b + 1) * LANES, :] = block.T.astype(BF16)
    loads[2].wait()
    for s in range(N // step):
        cols = pl.ds(s * step, step)
        high, low = split(0.25 * om_in[:, cols])
        om[0:rank, cols] = high
        om[rank : 2 * rank, cols] = low

    def sketch_copy(rc, t):
        return remote(
            sk_src.at[rc], sk_all.at[mc, rc], sk_ss.at[rc, t], sk_rs.at[rc, t], "col", lax.rem(mc + t, C)
        )

    def squared(u, right):
        return lax.dot_general(
            colf[u * UNIT : (u + 1) * UNIT, 0:16], right, NN, preferred_element_type=F32
        )

    for u in range(LEAD):
        sq[u][...] = squared(u, rowf[:, 0:chunk])

    def row_chunk(rc, carry):
        start = pl.multiple_of(rc * chunk, chunk)
        right = rowf[:, pl.ds(start, chunk)]
        right_next = rowf[:, pl.ds(pl.multiple_of(lax.rem(rc + 1, chunks) * chunk, chunk), chunk)]

        def use(u, acc):
            o = om[:, u * UNIT : (u + 1) * UNIT]
            for stage, whole in ((hi, khi), (lo, klo)):
                tile = jnp.concatenate([stage[u % 2][q] for q in range(chunk // LANES)], axis=1)
                acc = acc + lax.dot_general(o, tile, NN, preferred_element_type=F32)
                for q in range(chunk // LANES):
                    for p in range(UNIT // LANES):
                        whole[u * (UNIT // LANES) + p, pl.ds(start + q * LANES, LANES), :] = (
                            stage[u % 2][q, p * LANES : (p + 1) * LANES, :].T
                        )
            return acc

        acc = jnp.zeros((2 * rank, chunk), F32)
        for u in range(units):
            ahead = u + LEAD
            sq[ahead % BUFS][...] = squared(ahead % units, right if ahead < units else right_next)
            if u > 0:
                acc = use(u - 1, acc)
            for s in range(UNIT // SLICE):
                rows = slice(s * SLICE, (s + 1) * SLICE)
                value = jnp.maximum(sq[u % BUFS][rows, :], 1e-30)
                value = jnp.exp2((value * RATE) * lax.rsqrt(value))
                high, low = split(value)
                for q in range(chunk // LANES):
                    hi[u % 2][q, rows, :] = high[:, q * LANES : (q + 1) * LANES]
                    lo[u % 2][q, rows, :] = low[:, q * LANES : (q + 1) * LANES]
        acc = use(units - 1, acc)
        total = acc[:rank] + acc[rank:]

        @pl.when(rc == 0)
        def _():
            pl.semaphore_wait(barrier, R - 1 + C - 1)

        sk_src[rc] = total
        sk_all[mc, rc] = total
        for t in range(1, C):
            sketch_copy(rc, t).start()
        return carry

    lax.fori_loop(0, chunks, row_chunk, 0)

    for rc in range(chunks):
        for t in range(1, C):
            sketch_copy(rc, t).wait_recv()
    pieces = []
    for rc in range(chunks):
        total = sk_all[0, rc]
        for c in range(1, C):
            total = total + sk_all[c, rc]
        pieces.append(total)
    sketch = jnp.concatenate(pieces, axis=1)
    high, low = split(0.25 * sketch)
    sk_hl[0:rank, :] = high
    sk_hl[rank : 2 * rank, :] = low
    gram = lax.dot_general(sketch, sketch, NT, precision=HIGHEST, preferred_element_type=F32) / rows_total
    g_src[...] = jnp.zeros_like(g_src)
    g_src[:, rank : 2 * rank] = gram
    g_all[me] = g_src[...]

    def gram_copy(t):
        return remote(g_src, g_all.at[me], g_ss.at[t], g_rs.at[t], "row", row_of(t))

    for t in range(1, R):
        gram_copy(t).start()

    def pair_copy(t):
        return remote(wp.at[t, 1 - side], s_in.at[t], p_ss.at[t], p_rs.at[t], "row", sib)

    def w_copy(t):
        return remote(w_src.at[t], w_all.at[t], w_ss.at[t], w_rs.at[t], "row", 2 * chip_to(t) + side)

    tiles = 2 * part // LANES

    def product(t):
        base = chip_to(t) * tiles
        s = sk_hl[...]
        acc = None
        for whole in (khi, klo):
            block = jnp.concatenate([whole[base + i] for i in range(tiles)], axis=1)
            term = lax.dot_general(s, block, NN, preferred_element_type=F32)
            acc = term if acc is None else acc + term
        acc = acc[:rank] + acc[rank:]
        wp[t, 0] = acc[:, :part]
        wp[t, 1] = acc[:, part:]

    def forward(t):
        pair_copy(t).wait_recv()
        w_src[t] = wp[t, side] + s_in[t]
        w_copy(t).start()

    before = None
    for t in far_first:
        product(t)
        pair_copy(t).start()
        if before is not None:
            forward(before)
        before = t
    for t in range(1, R):
        gram_copy(t).wait_recv()
    product(0)
    mat = g_all[0]
    for r in range(1, R):
        mat = mat + g_all[r]
    sub = lax.broadcasted_iota(jnp.int32, mat.shape, 0)
    lane = lax.broadcasted_iota(jnp.int32, mat.shape, 1)
    mat = mat + jnp.where(lane == sub, 1.0, 0.0)
    for k in range(rank - 1):
        row = mat[k : k + 1, :]
        factor = mat[:, rank + k : rank + k + 1] * (1.0 / mat[k : k + 1, rank + k : rank + k + 1])
        mat = mat - jnp.where(sub > k, factor * row, 0.0)
    diag = jnp.sum(jnp.where(lane == sub + rank, mat, 0.0), axis=1, keepdims=True)
    inverse = (mat * (1.0 / jnp.sqrt(diag)))[:, :rank]
    inverse = jnp.where(lane[:, :rank] <= sub[:, :rank], inverse, 0.0)
    pair_copy(0).start()
    if before is not None:
        forward(before)
    basis_ref[...] = jnp.dot(inverse, sketch, precision=HIGHEST, preferred_element_type=F32)
    pair_copy(0).wait_recv()
    total = wp[0, side] + s_in[0]
    for t in far_first:
        w_copy(t).wait_recv()
        total = total + w_all[t]
    mine = jnp.dot(inverse, total, precision=HIGHEST, preferred_element_type=F32)
    img[me] = mine

    def far_copy(t):
        return remote(img.at[me], img.at[me], a_ss.at[t], a_rs.at[t], "row", 2 * chip_to(t) + side)

    def near_copy(t):
        slot = 2 * chip_from(t) + side
        return remote(img.at[slot], img.at[slot], f_ss.at[t], f_rs.at[t], "row", sib)

    def core_copy(t):
        return remote(c_src, c_all.at[me], c_ss.at[t], c_rs.at[t], "row", row_of(t))

    def last_copy(t):
        return remote(d_src, d_all.at[mc], d_ss.at[t], d_rs.at[t], "col", lax.rem(mc + t, C))

    core = lax.dot_general(mine, mine, NT, precision=HIGHEST, preferred_element_type=F32) / order
    c_src[...] = jnp.zeros_like(c_src)
    c_src[:, 0:rank] = core
    c_all[me] = c_src[...]
    for t in range(1, R):
        core_copy(t).start()
    for t in far_first:
        far_copy(t).start()
    near_copy(0).start()
    for t in range(1, R):
        core_copy(t).wait_recv()
    core = c_all[0]
    for r in range(1, R):
        core = core + c_all[r]
    d_src[...] = core
    d_all[mc] = core
    for t in range(1, C):
        last_copy(t).start()
    for t in reversed(far_first):
        far_copy(t).wait_recv()
        near_copy(t).start()
    for t in range(half):
        near_copy(t).wait_recv()
    for r in range(R):
        image_ref[:, r * part : (r + 1) * part] = img[r]
    for t in range(1, C):
        last_copy(t).wait_recv()
    core = d_all[0]
    for c in range(1, C):
        core = core + d_all[c]
    core_ref[...] = core[:, 0:rank]

    for rc in range(chunks):
        for t in range(1, C):
            sketch_copy(rc, t).wait_send()
    for t in range(1, R):
        gram_copy(t).wait_send()
        core_copy(t).wait_send()
    for t in range(half):
        pair_copy(t).wait_send()
        near_copy(t).wait_send()
    for t in far_first:
        w_copy(t).wait_send()
        far_copy(t).wait_send()
    for t in range(1, C):
        last_copy(t).wait_send()


def finish(*refs):
    copies = [pltpu.make_async_copy(refs[i], refs[3 + i], refs[6].at[i]) for i in range(3)]
    for copy in copies:
        copy.start()
    for copy in copies:
        copy.wait()


def shards(row_cells, col_cells, omega):
    R, C = lax.axis_size("row"), lax.axis_size("col")
    rank = omega.shape[0]
    M, N = row_cells.shape[1], col_cells.shape[1]
    chunk = min(M, UNIT)
    chunks, part, half = M // chunk, N // R, R // 2
    shape = (R, C, rank, M, N, M * R, N * C)
    vmem = pltpu.VMEM
    dma = pltpu.SemaphoreType.DMA
    full = pl.BlockSpec(memory_space=pltpu.VMEM)
    hbm = pl.BlockSpec(memory_space=pltpu.HBM)
    out_shape = (
        jax.ShapeDtypeStruct((rank, M), F32),
        jax.ShapeDtypeStruct((rank, N), F32),
        jax.ShapeDtypeStruct((rank, rank), F32),
    )
    outs = pl.pallas_call(
        functools.partial(kernel, shape),
        out_shape=out_shape,
        in_specs=[hbm] * 3,
        out_specs=(full,) * 3,
        scratch_shapes=[
            vmem(row_cells.shape, jnp.int32),
            vmem(col_cells.shape, jnp.int32),
            vmem((rank, N), F32),
            vmem((16, M), BF16),
            vmem((N, LANES), BF16),
            vmem((2 * rank, N), BF16),
            vmem((N // LANES, M, LANES), BF16),
            vmem((N // LANES, M, LANES), BF16),
            *[vmem((UNIT, chunk), F32)] * BUFS,
            *[vmem((chunk // LANES, UNIT, LANES), BF16)] * 4,
            vmem((chunks, rank, chunk), F32),
            vmem((C, chunks, rank, chunk), F32),
            vmem((2 * rank, M), BF16),
            vmem((rank, LANES), F32),
            vmem((R, rank, LANES), F32),
            vmem((half, 2, rank, part), F32),
            vmem((half, rank, part), F32),
            vmem((half, rank, part), F32),
            vmem((half, rank, part), F32),
            vmem((R, rank, part), F32),
            vmem((rank, LANES), F32),
            vmem((R, rank, LANES), F32),
            vmem((rank, LANES), F32),
            vmem((C, rank, LANES), F32),
            dma((3,)),
            dma((chunks, C)), dma((chunks, C)),
            dma((R,)), dma((R,)),
            dma((half,)), dma((half,)),
            dma((half,)), dma((half,)),
            dma((half,)), dma((half,)),
            dma((half,)), dma((half,)),
            dma((R,)), dma((R,)),
            dma((C,)), dma((C,)),
        ],
        compiler_params=pltpu.CompilerParams(
            collective_id=0, has_side_effects=True, vmem_limit_bytes=48 * 1024 * 1024
        ),
    )(row_cells, col_cells, omega)
    return pl.pallas_call(
        finish,
        out_shape=out_shape,
        in_specs=[full] * 3,
        out_specs=(hbm,) * 3,
        scratch_shapes=[dma((3,))],
        compiler_params=pltpu.CompilerParams(vmem_limit_bytes=4 * 1024 * 1024),
    )(*outs)


def solution(mesh):
    return jax.shard_map(
        shards,
        mesh=mesh,
        in_specs=(P(None, "row"), P(None, "col"), P(None, "col")),
        out_specs=(P(None, "row"), P(None, "col"), P()),
        check_vma=False,
    )
```

```python
import functools
import math

import jax
import jax.numpy as jnp
from jax import lax
from jax.experimental import pallas as pl
from jax.experimental.pallas import tpu as pltpu
from jax.sharding import PartitionSpec as P

BF16, F32 = jnp.bfloat16, jnp.float32
HIGHEST = lax.Precision.HIGHEST
NT = (((1,), (1,)), ((), ()))
NN = (((1,), (0,)), ((), ()))
LANES = 128
RATE = -math.log2(math.e) / 6.4
UNIT = 256
LEAD = 3
BUFS = 4
SLICE = 64
VMEM_LIMIT = 48000 * 1024


def split(x):
    high = x.astype(BF16)
    return high, (x - high.astype(F32)).astype(BF16)


def loop(first, last, body):
    if last - first < 64:
        for k in range(first, last):
            body(k, 0)
    else:
        lax.fori_loop(first, last, body, 0)


def features(cells, left):
    x = [cells[d : d + 1, :].astype(F32) - 32.0 for d in range(3)]
    norm = x[0] * x[0] + x[1] * x[1] + x[2] * x[2]
    high = jnp.floor(norm * 0.0625) * 16.0
    low = norm - high
    one, zero = jnp.ones_like(norm), jnp.zeros_like(norm)
    if left:
        rows = [-2.0 * x[0], -2.0 * x[1], -2.0 * x[2], one, one, high, low, zero]
    else:
        rows = [x[0], x[1], x[2], high, low, one, one, zero]
    return jnp.concatenate(rows, axis=0)


def kernel(
    shape,
    row_hbm, col_hbm, omega_hbm,
    basis_ref, image_ref, core_ref,
    row_in, col_in, om_in, rowf, colf, om, khi, klo, sq0, sq1, sq2, sq3, hi0, hi1, lo0, lo1,
    sk_src, sk_all, sk_hl, g_src, g_all, wacc, wp, s_in, w_src, w_all, img, c_src, c_all,
    in_s, sk_rs, p_rs, a_rs, one_s,
):
    R, C, rank, M, N, rows_total, order = shape
    me = lax.axis_index("row")
    mc = lax.axis_index("col")
    half = R // 2
    side = lax.rem(me, 2)
    chip = me // 2
    sib = me + 1 - 2 * side
    part = N // R
    chunk = min(M, UNIT)
    chunks = M // chunk
    group = max(chunks // 2, 1)
    groups = chunks // group
    devices = R * C
    index = mc * R + me
    units = N // UNIT
    sq = (sq0, sq1, sq2, sq3)
    hi, lo = (hi0, hi1), (lo0, lo1)
    binary = half & (half - 1) == 0
    far_first = sorted(range(1, half), key=lambda t: -bin(t).count("1"))

    def row_of(t):
        return lax.rem(me + t, R)

    def chip_to(t):
        if not binary:
            return lax.rem(chip + t, half)
        total, bit = 0, 1
        while bit < half:
            total = total + bit * lax.rem(chip // bit + t // bit, 2)
            bit *= 2
        return total

    def chip_from(t):
        return chip_to(t) if binary else lax.rem(chip + half - t, half)

    def remote(src, dst, ss, rs, axis, peer):
        return pltpu.make_async_remote_copy(
            src_ref=src, dst_ref=dst, send_sem=ss, recv_sem=rs,
            device_id={axis: peer}, device_id_type=pl.DeviceIdType.MESH,
        )

    sk_ss, g_ss, g_rs, p_ss, w_ss, w_rs, a_ss, f_ss, f_rs, c_ss, c_rs = (one_s.at[i] for i in range(11))

    def all_sent(ref, ss):
        remote(ref, ref, ss, ss, "row", sib).wait_send()

    def all_received(ref, rs):
        remote(ref, ref, rs, rs, "row", sib).wait_recv()

    loads = [
        pltpu.make_async_copy(source, target, in_s.at[i])
        for i, (source, target) in enumerate(((col_hbm, col_in), (row_hbm, row_in), (omega_hbm, om_in)))
    ]
    for load in loads:
        load.start()
    barrier = pltpu.get_barrier_semaphore()

    def peer(k):
        other = lax.rem(index + k, devices)
        return {"row": lax.rem(other, R), "col": other // R}

    def greet(k, carry):
        pl.semaphore_signal(barrier, inc=1, device_id=peer(k), device_id_type=pl.DeviceIdType.MESH)
        return carry

    loop(1, devices, greet)

    loads[0].wait()
    loads[1].wait()
    rowf[0:8, :] = features(row_in[...], False).astype(BF16)
    rowf[8:16, :] = jnp.zeros((8, M), BF16)
    step = min(N, 1024)
    for s in range(N // step):
        left = features(col_in[:, s * step : (s + 1) * step], True)
        for b in range(step // LANES):
            block = jnp.concatenate(
                [left[:, b * LANES : (b + 1) * LANES], jnp.zeros((LANES - 8, LANES), F32)], axis=0
            )
            colf[s * step + b * LANES : s * step + (b + 1) * LANES, :] = block.T.astype(BF16)
    loads[2].wait()
    for s in range(N // step):
        cols = pl.ds(s * step, step)
        high, low = split(0.25 * om_in[:, cols])
        om[0:rank, cols] = high
        om[rank : 2 * rank, cols] = low

    def sketch_copy(rc, t):
        return remote(
            sk_src.at[rc], sk_all.at[mc, rc], sk_ss, sk_rs.at[rc // group], "col", lax.rem(mc + t, C)
        )

    def squared(u, right):
        return lax.dot_general(
            colf[u * UNIT : (u + 1) * UNIT, 0:16], right, NN, preferred_element_type=F32
        )

    for u in range(LEAD):
        sq[u][...] = squared(u, rowf[:, 0:chunk])

    def row_chunk(rc, carry):
        start = pl.multiple_of(rc * chunk, chunk)
        right = rowf[:, pl.ds(start, chunk)]
        right_next = rowf[:, pl.ds(pl.multiple_of(lax.rem(rc + 1, chunks) * chunk, chunk), chunk)]

        def use(u, acc):
            o = om[:, u * UNIT : (u + 1) * UNIT]
            for stage, whole in ((hi, khi), (lo, klo)):
                tile = jnp.concatenate([stage[u % 2][q] for q in range(chunk // LANES)], axis=1)
                acc = acc + lax.dot_general(o, tile, NN, preferred_element_type=F32)
                for q in range(chunk // LANES):
                    for p in range(UNIT // LANES):
                        whole[u * (UNIT // LANES) + p, pl.ds(start + q * LANES, LANES), :] = (
                            stage[u % 2][q, p * LANES : (p + 1) * LANES, :].T
                        )
            return acc

        acc = jnp.zeros((2 * rank, chunk), F32)
        for u in range(units):
            ahead = u + LEAD
            sq[ahead % BUFS][...] = squared(ahead % units, right if ahead < units else right_next)
            if u > 0:
                acc = use(u - 1, acc)
            for s in range(UNIT // SLICE):
                rows = slice(s * SLICE, (s + 1) * SLICE)
                value = jnp.maximum(sq[u % BUFS][rows, :], 1e-30)
                value = jnp.exp2((value * RATE) * lax.rsqrt(value))
                high, low = split(value)
                for q in range(chunk // LANES):
                    hi[u % 2][q, rows, :] = high[:, q * LANES : (q + 1) * LANES]
                    lo[u % 2][q, rows, :] = low[:, q * LANES : (q + 1) * LANES]
        acc = use(units - 1, acc)
        total = acc[:rank] + acc[rank:]

        @pl.when(rc == 0)
        def _():
            pl.semaphore_wait(barrier, devices - 1)

        sk_src[rc] = total
        sk_all[mc, rc] = total
        for t in range(1, C):
            sketch_copy(rc, t).start()
        return carry

    lax.fori_loop(0, chunks, row_chunk, 0)

    tiles = 2 * part // LANES

    def product(base, g):
        rows = slice(g * group * chunk, (g + 1) * group * chunk)
        s = sk_hl[:, rows]
        acc = None
        for whole in (khi, klo):
            block = jnp.concatenate([whole[base + i, rows, :] for i in range(tiles)], axis=1)
            term = lax.dot_general(s, block, NN, preferred_element_type=F32)
            acc = term if acc is None else acc + term
        return acc[:rank] + acc[rank:]

    def take(g):
        if C > 1:
            all_received(sk_all.at[pl.ds(0, C - 1), pl.ds(0, group)], sk_rs.at[g])
        pieces = []
        for rc in range(g * group, (g + 1) * group):
            total = sk_all[0, rc]
            for c in range(1, C):
                total = total + sk_all[c, rc]
            pieces.append(total)
        sketch = jnp.concatenate(pieces, axis=1)
        high, low = split(0.25 * sketch)
        rows = slice(g * group * chunk, (g + 1) * group * chunk)
        sk_hl[0:rank, rows] = high
        sk_hl[rank : 2 * rank, rows] = low
        return sketch, lax.dot_general(sketch, sketch, NT, precision=HIGHEST, preferred_element_type=F32)

    parts, gram = [], None
    for g in range(groups):
        some, term = take(g)
        parts.append(some)
        gram = term if gram is None else gram + term
        if g == groups - 1:
            break

        def early(b, carry):
            acc = product(b * tiles, g)
            if g > 0:
                acc = acc + wacc[b]
            wacc[b] = acc
            return carry

        loop(0, half, early)
    sketch = jnp.concatenate(parts, axis=1)
    g_src[...] = jnp.zeros_like(g_src)
    g_src[:, rank : 2 * rank] = gram / rows_total
    g_all[me] = g_src[...]

    def gram_copy(t):
        return remote(g_src, g_all.at[me], g_ss, g_rs, "row", row_of(t))

    for t in range(1, R):
        gram_copy(t).start()

    def pair_copy(t):
        return remote(wp.at[t, 1 - side], s_in.at[t], p_ss, p_rs.at[t], "row", sib)

    def w_copy(t):
        return remote(w_src.at[t], w_all.at[t], w_ss, w_rs, "row", 2 * chip_to(t) + side)

    def blocks(t):
        to = chip_to(t)
        acc = product(to * tiles, groups - 1)
        if groups > 1:
            acc = acc + wacc[to]
        wp[t, 0] = acc[:, :part]
        wp[t, 1] = acc[:, part:]

    def forward(t):
        pair_copy(t).wait_recv()
        w_src[t] = wp[t, side] + s_in[t]
        w_copy(t).start()

    before = None
    for t in far_first:
        blocks(t)
        pair_copy(t).start()
        if before is not None:
            forward(before)
        before = t
    blocks(0)
    pair_copy(0).start()
    if before is not None:
        forward(before)
    all_received(g_all.at[pl.ds(0, R - 1)], g_rs)
    mat = g_all[0]
    for r in range(1, R):
        mat = mat + g_all[r]
    sub = lax.broadcasted_iota(jnp.int32, mat.shape, 0)
    lane = lax.broadcasted_iota(jnp.int32, mat.shape, 1)
    mat = mat + jnp.where(lane == sub, 1.0, 0.0)
    for k in range(rank - 1):
        row = mat[k : k + 1, :]
        factor = mat[:, rank + k : rank + k + 1] * (1.0 / mat[k : k + 1, rank + k : rank + k + 1])
        mat = mat - jnp.where(sub > k, factor * row, 0.0)
    diag = jnp.sum(jnp.where(lane == sub + rank, mat, 0.0), axis=1, keepdims=True)
    inverse = (mat * (1.0 / jnp.sqrt(diag)))[:, :rank]
    inverse = jnp.where(lane[:, :rank] <= sub[:, :rank], inverse, 0.0)
    basis_ref[...] = jnp.dot(inverse, sketch, precision=HIGHEST, preferred_element_type=F32)
    pair_copy(0).wait_recv()
    total = wp[0, side] + s_in[0]
    if half > 1:
        all_received(w_all.at[pl.ds(0, half - 1)], w_rs)
    for t in far_first:
        total = total + w_all[t]
    mine = jnp.dot(inverse, total, precision=HIGHEST, preferred_element_type=F32)
    img[me] = mine

    def far_copy(t):
        return remote(img.at[me], img.at[me], a_ss, a_rs.at[t], "row", 2 * chip_to(t) + side)

    def near_copy(t):
        slot = 2 * chip_from(t) + side
        return remote(img.at[slot], img.at[slot], f_ss, f_rs, "row", sib)

    def core_copy(k):
        return pltpu.make_async_remote_copy(
            src_ref=c_src, dst_ref=c_all.at[index], send_sem=c_ss, recv_sem=c_rs,
            device_id=peer(k), device_id_type=pl.DeviceIdType.MESH,
        )

    per_row = LANES // rank
    packed = rank // per_row
    sub = lax.broadcasted_iota(jnp.int32, (rank, LANES), 0)
    lane = lax.broadcasted_iota(jnp.int32, (rank, LANES), 1)
    own = lane // rank == lax.rem(sub, per_row)

    both = jnp.concatenate(split(mine), axis=0)
    core = lax.dot_general(both, both, NT, preferred_element_type=F32) / order
    core = core[:rank] + core[rank:]
    core = core[:, :rank] + core[:, rank:]
    wide = jnp.where(own, jnp.concatenate([core] * per_row, axis=1), 0.0)
    flat = jnp.concatenate(
        [jnp.sum(wide[a * per_row : (a + 1) * per_row, :], axis=0, keepdims=True) for a in range(packed)], axis=0
    )
    c_src[...] = flat
    c_all[index] = flat

    def send_core(k, carry):
        core_copy(k).start()
        return carry

    loop(1, devices, send_core)
    for t in far_first:
        far_copy(t).start()
    near_copy(0).start()
    for t in reversed(far_first):
        far_copy(t).wait_recv()
        near_copy(t).start()
    all_received(img.at[pl.ds(0, half)], f_rs)
    for r in range(R):
        image_ref[:, r * part : (r + 1) * part] = img[r]
    all_received(c_all.at[pl.ds(0, devices - 1)], c_rs)
    flat = jnp.sum(c_all[...], axis=0)
    wide = jnp.concatenate(
        [jnp.broadcast_to(flat[a : a + 1, :], (per_row, LANES)) for a in range(packed)], axis=0
    )
    wide = jnp.where(own, wide, 0.0)
    shift = LANES // 2
    while shift >= rank:
        wide = wide + pltpu.roll(wide, shift, 1)
        shift //= 2
    core_ref[...] = wide[:, 0:rank]

    if C > 1:
        all_sent(sk_all.at[pl.ds(0, C - 1)], sk_ss)
    all_sent(g_all.at[pl.ds(0, R - 1)], g_ss)
    all_sent(s_in, p_ss)
    if half > 1:
        all_sent(w_all.at[pl.ds(0, half - 1)], w_ss)
        all_sent(img.at[pl.ds(0, half - 1)], a_ss)
    all_sent(img.at[pl.ds(0, half)], f_ss)
    all_sent(c_all.at[pl.ds(0, devices - 1)], c_ss)


def finish(*refs):
    copies = [pltpu.make_async_copy(refs[i], refs[3 + i], refs[6].at[i]) for i in range(3)]
    for copy in copies:
        copy.start()
    for copy in copies:
        copy.wait()


def shards(row_cells, col_cells, omega):
    R, C = lax.axis_size("row"), lax.axis_size("col")
    rank = omega.shape[0]
    M, N = row_cells.shape[1], col_cells.shape[1]
    chunk = min(M, UNIT)
    chunks, part, half = M // chunk, N // R, R // 2
    groups = chunks // max(chunks // 2, 1)
    shape = (R, C, rank, M, N, M * R, N * C)
    vmem = pltpu.VMEM
    dma = pltpu.SemaphoreType.DMA
    full = pl.BlockSpec(memory_space=pltpu.VMEM)
    hbm = pl.BlockSpec(memory_space=pltpu.HBM)
    out_shape = (
        jax.ShapeDtypeStruct((rank, M), F32),
        jax.ShapeDtypeStruct((rank, N), F32),
        jax.ShapeDtypeStruct((rank, rank), F32),
    )
    outs = pl.pallas_call(
        functools.partial(kernel, shape),
        out_shape=out_shape,
        in_specs=[hbm] * 3,
        out_specs=(full,) * 3,
        scratch_shapes=[
            vmem(row_cells.shape, jnp.int32),
            vmem(col_cells.shape, jnp.int32),
            vmem((rank, N), F32),
            vmem((16, M), BF16),
            vmem((N, LANES), BF16),
            vmem((2 * rank, N), BF16),
            vmem((N // LANES, M, LANES), BF16),
            vmem((N // LANES, M, LANES), BF16),
            *[vmem((UNIT, chunk), F32)] * BUFS,
            *[vmem((chunk // LANES, UNIT, LANES), BF16)] * 4,
            vmem((chunks, rank, chunk), F32),
            vmem((C, chunks, rank, chunk), F32),
            vmem((2 * rank, M), BF16),
            vmem((rank, LANES), F32),
            vmem((R, rank, LANES), F32),
            vmem((half, rank, 2 * part), F32),
            vmem((half, 2, rank, part), F32),
            vmem((half, rank, part), F32),
            vmem((half, rank, part), F32),
            vmem((half, rank, part), F32),
            vmem((R, rank, part), F32),
            vmem((rank * rank // LANES, LANES), F32),
            vmem((R * C, rank * rank // LANES, LANES), F32),
            dma((3,)), dma((groups,)), dma((half,)), dma((half,)), dma((11,)),
        ],
        compiler_params=pltpu.CompilerParams(
            collective_id=0, has_side_effects=True, vmem_limit_bytes=VMEM_LIMIT
        ),
    )(*(pltpu.with_memory_space_constraint(x, pltpu.HBM) for x in (row_cells, col_cells, omega)))
    return pl.pallas_call(
        finish,
        out_shape=out_shape,
        in_specs=[full] * 3,
        out_specs=(hbm,) * 3,
        scratch_shapes=[dma((3,))],
        compiler_params=pltpu.CompilerParams(vmem_limit_bytes=4 * 1024 * 1024),
    )(*outs)


def solution(mesh):
    return jax.shard_map(
        shards,
        mesh=mesh,
        in_specs=(P(None, "row"), P(None, "col"), P(None, "col")),
        out_specs=(P(None, "row"), P(None, "col"), P()),
        check_vma=False,
    )
```

```python
import functools
import math

import jax
import jax.numpy as jnp
from jax import lax
from jax.experimental import pallas as pl
from jax.experimental.pallas import tpu as pltpu
from jax.sharding import PartitionSpec as P

BF16, F32 = jnp.bfloat16, jnp.float32
HIGHEST = lax.Precision.HIGHEST
NT = (((1,), (1,)), ((), ()))
NN = (((1,), (0,)), ((), ()))
LANES = 128
RATE = -math.log2(math.e) / 6.4
UNIT = 256
LEAD = 3
BUFS = 4
SLICE = 64
VMEM_LIMIT = 48000 * 1024


def split(x):
    high = x.astype(BF16)
    return high, (x - high.astype(F32)).astype(BF16)


def loop(first, last, body):
    if last - first < 64:
        for k in range(first, last):
            body(k, 0)
    else:
        lax.fori_loop(first, last, body, 0)


def features(cells, left):
    x = [cells[d : d + 1, :].astype(F32) - 32.0 for d in range(3)]
    norm = x[0] * x[0] + x[1] * x[1] + x[2] * x[2]
    high = jnp.floor(norm * 0.0625) * 16.0
    low = norm - high
    one, zero = jnp.ones_like(norm), jnp.zeros_like(norm)
    if left:
        rows = [-2.0 * x[0], -2.0 * x[1], -2.0 * x[2], one, one, high, low, zero]
    else:
        rows = [x[0], x[1], x[2], high, low, one, one, zero]
    return jnp.concatenate(rows, axis=0)


def kernel(
    shape,
    row_hbm, col_hbm, omega_hbm,
    basis_ref, image_ref, core_ref,
    row_in, col_in, om_in, rowf, colf, om, khi, klo, sq0, sq1, sq2, sq3, hi0, hi1, lo0, lo1,
    sk_src, sk_all, sk_hl, g_src, g_all, wacc, wp, s_in, w_src, w_all, img, c_src, c_all,
    in_s, sk_rs, p_rs, a_rs, one_s,
):
    R, C, rank, M, N, rows_total, order = shape
    me = lax.axis_index("row")
    mc = lax.axis_index("col")
    half = R // 2
    side = lax.rem(me, 2)
    chip = me // 2
    sib = me + 1 - 2 * side
    part = N // R
    chunk = min(M, UNIT)
    chunks = M // chunk
    group = max(chunks // 2, 1)
    groups = chunks // group
    devices = R * C
    index = mc * R + me
    units = N // UNIT
    sq = (sq0, sq1, sq2, sq3)
    hi, lo = (hi0, hi1), (lo0, lo1)
    binary = half & (half - 1) == 0
    far_first = sorted(range(1, half), key=lambda t: -bin(t).count("1"))

    def row_of(t):
        return lax.rem(me + t, R)

    def chip_to(t):
        if not binary:
            return lax.rem(chip + t, half)
        total, bit = 0, 1
        while bit < half:
            total = total + bit * lax.rem(chip // bit + t // bit, 2)
            bit *= 2
        return total

    def chip_from(t):
        return chip_to(t) if binary else lax.rem(chip + half - t, half)

    def remote(src, dst, ss, rs, axis, peer):
        return pltpu.make_async_remote_copy(
            src_ref=src, dst_ref=dst, send_sem=ss, recv_sem=rs,
            device_id={axis: peer}, device_id_type=pl.DeviceIdType.MESH,
        )

    sk_ss, g_ss, g_rs, p_ss, w_ss, w_rs, a_ss, f_ss, f_rs, c_ss, c_rs = (one_s.at[i] for i in range(11))

    def all_sent(ref, ss):
        remote(ref, ref, ss, ss, "row", sib).wait_send()

    def all_received(ref, rs):
        remote(ref, ref, rs, rs, "row", sib).wait_recv()

    loads = [
        pltpu.make_async_copy(source, target, in_s.at[i])
        for i, (source, target) in enumerate(((col_hbm, col_in), (row_hbm, row_in), (omega_hbm, om_in)))
    ]
    for load in loads:
        load.start()
    barrier = pltpu.get_barrier_semaphore()

    def peer(k):
        other = lax.rem(index + k, devices)
        return {"row": lax.rem(other, R), "col": other // R}

    def greet(k, carry):
        pl.semaphore_signal(barrier, inc=1, device_id=peer(k), device_id_type=pl.DeviceIdType.MESH)
        return carry

    loop(1, devices, greet)

    loads[0].wait()
    loads[1].wait()
    rowf[0:8, :] = features(row_in[...], False).astype(BF16)
    rowf[8:16, :] = jnp.zeros((8, M), BF16)
    step = min(N, 1024)
    for s in range(N // step):
        left = features(col_in[:, s * step : (s + 1) * step], True)
        left = jnp.concatenate([left, jnp.zeros((8, step), F32)], axis=0).astype(BF16)
        for b in range(step // LANES):
            block = jnp.concatenate(
                [left[:, b * LANES : (b + 1) * LANES], jnp.zeros((LANES - 16, LANES), BF16)], axis=0
            )
            colf[s * step + b * LANES : s * step + (b + 1) * LANES, :] = block.T
    loads[2].wait()
    for s in range(N // step):
        cols = pl.ds(s * step, step)
        high, low = split(0.25 * om_in[:, cols])
        om[0:rank, cols] = high
        om[rank : 2 * rank, cols] = low

    def sketch_copy(rc, t):
        return remote(
            sk_src.at[rc], sk_all.at[mc, rc], sk_ss, sk_rs.at[rc // group], "col", lax.rem(mc + t, C)
        )

    def squared(u, right):
        return lax.dot_general(
            colf[u * UNIT : (u + 1) * UNIT, 0:16], right, NN, preferred_element_type=F32
        )

    for u in range(LEAD):
        sq[u][...] = squared(u, rowf[:, 0:chunk])

    def row_chunk(rc, carry):
        start = pl.multiple_of(rc * chunk, chunk)
        right = rowf[:, pl.ds(start, chunk)]
        right_next = rowf[:, pl.ds(pl.multiple_of(lax.rem(rc + 1, chunks) * chunk, chunk), chunk)]

        def use(u, acc):
            o = om[:, u * UNIT : (u + 1) * UNIT]
            for stage, whole in ((hi, khi), (lo, klo)):
                tile = jnp.concatenate([stage[u % 2][q] for q in range(chunk // LANES)], axis=1)
                acc = acc + lax.dot_general(o, tile, NN, preferred_element_type=F32)
                for q in range(chunk // LANES):
                    for p in range(UNIT // LANES):
                        whole[u * (UNIT // LANES) + p, pl.ds(start + q * LANES, LANES), :] = (
                            stage[u % 2][q, p * LANES : (p + 1) * LANES, :].T
                        )
            return acc

        acc = jnp.zeros((2 * rank, chunk), F32)
        for u in range(units):
            ahead = u + LEAD
            sq[ahead % BUFS][...] = squared(ahead % units, right if ahead < units else right_next)
            if u > 0:
                acc = use(u - 1, acc)
            for s in range(UNIT // SLICE):
                rows = slice(s * SLICE, (s + 1) * SLICE)
                value = jnp.maximum(sq[u % BUFS][rows, :], 1e-30)
                value = jnp.exp2((value * RATE) * lax.rsqrt(value))
                high, low = split(value)
                for q in range(chunk // LANES):
                    hi[u % 2][q, rows, :] = high[:, q * LANES : (q + 1) * LANES]
                    lo[u % 2][q, rows, :] = low[:, q * LANES : (q + 1) * LANES]
        acc = use(units - 1, acc)
        total = acc[:rank] + acc[rank:]

        @pl.when(rc == 0)
        def _():
            pl.semaphore_wait(barrier, devices - 1)

        sk_src[rc] = total
        sk_all[mc, rc] = total
        for t in range(1, C):
            sketch_copy(rc, t).start()
        return carry

    lax.fori_loop(0, chunks, row_chunk, 0)

    tiles = 2 * part // LANES

    def product(base, g, count):
        rows = slice(g * group * chunk, (g + 1) * group * chunk)
        s = sk_hl[:, rows]
        acc = None
        for whole in (khi, klo):
            block = jnp.concatenate([whole[base + i, rows, :] for i in range(count)], axis=1)
            term = lax.dot_general(s, block, NN, preferred_element_type=F32)
            acc = term if acc is None else acc + term
        return acc[:rank] + acc[rank:]

    def take(g):
        if C > 1:
            all_received(sk_all.at[pl.ds(0, C - 1), pl.ds(0, group)], sk_rs.at[g])
        pieces = []
        for rc in range(g * group, (g + 1) * group):
            total = sk_all[0, rc]
            for c in range(1, C):
                total = total + sk_all[c, rc]
            pieces.append(total)
        sketch = jnp.concatenate(pieces, axis=1)
        high, low = split(0.25 * sketch)
        rows = slice(g * group * chunk, (g + 1) * group * chunk)
        sk_hl[0:rank, rows] = high
        sk_hl[rank : 2 * rank, rows] = low
        return sketch, lax.dot_general(sketch, sketch, NT, precision=HIGHEST, preferred_element_type=F32)

    def early(t, g):
        to = chip_to(t)
        acc = product(to * tiles, g, tiles)
        for which in range(2):
            some = acc[:, which * part : (which + 1) * part]
            wacc[to, which] = some if g == 0 else some + wacc[to, which]

    parts, gram = [], None
    for g in range(groups):
        some, term = take(g)
        parts.append(some)
        gram = term if gram is None else gram + term
        if g == groups - 1:
            break

        for t in far_first:
            early(t, g)
    sketch = jnp.concatenate(parts, axis=1)
    g_src[...] = jnp.zeros_like(g_src)
    g_src[:, rank : 2 * rank] = gram / rows_total
    g_all[me] = g_src[...]

    def gram_copy(t):
        return remote(g_src, g_all.at[me], g_ss, g_rs, "row", row_of(t))

    for t in range(1, R):
        gram_copy(t).start()

    def pair_copy(t):
        return remote(wp.at[t, 1 - side], s_in.at[t], p_ss, p_rs.at[t], "row", sib)

    def w_copy(t):
        return remote(w_src.at[t], w_all.at[t], w_ss, w_rs, "row", 2 * chip_to(t) + side)

    def blocks(t):
        to = chip_to(t)
        for which in (1 - side, side):
            acc = product(to * tiles + which * (tiles // 2), groups - 1, tiles // 2)
            if groups > 1:
                acc = acc + wacc[to, which]
            wp[t, which] = acc
            if which is not side:
                pair_copy(t).start()

    def forward(t):
        pair_copy(t).wait_recv()
        w_src[t] = wp[t, side] + s_in[t]
        w_copy(t).start()

    before = None
    for t in far_first:
        blocks(t)
        if before is not None:
            forward(before)
        before = t
    for g in range(groups - 1):
        early(0, g)
    if before is not None:
        forward(before)
    all_received(g_all.at[pl.ds(0, R - 1)], g_rs)
    blocks(0)
    mat = g_all[0]
    for r in range(1, R):
        mat = mat + g_all[r]
    sub = lax.broadcasted_iota(jnp.int32, mat.shape, 0)
    lane = lax.broadcasted_iota(jnp.int32, mat.shape, 1)
    mat = mat + jnp.where(lane == sub, 1.0, 0.0)
    for k in range(rank - 1):
        row = mat[k : k + 1, :]
        factor = mat[:, rank + k : rank + k + 1] * (1.0 / mat[k : k + 1, rank + k : rank + k + 1])
        mat = mat - jnp.where(sub > k, factor * row, 0.0)
    diag = jnp.sum(jnp.where(lane == sub + rank, mat, 0.0), axis=1, keepdims=True)
    inverse = (mat * (1.0 / jnp.sqrt(diag)))[:, :rank]
    inverse = jnp.where(lane[:, :rank] <= sub[:, :rank], inverse, 0.0)
    basis_ref[...] = jnp.dot(inverse, sketch, precision=HIGHEST, preferred_element_type=F32)
    pair_copy(0).wait_recv()
    total = wp[0, side] + s_in[0]
    if half > 1:
        all_received(w_all.at[pl.ds(0, half - 1)], w_rs)
    for t in far_first:
        total = total + w_all[t]
    mine = jnp.dot(inverse, total, precision=HIGHEST, preferred_element_type=F32)
    img[me] = mine

    def far_copy(t):
        return remote(img.at[me], img.at[me], a_ss, a_rs.at[t], "row", 2 * chip_to(t) + side)

    def near_copy(t):
        slot = 2 * chip_from(t) + side
        return remote(img.at[slot], img.at[slot], f_ss, f_rs, "row", sib)

    def core_copy(k):
        return pltpu.make_async_remote_copy(
            src_ref=c_src, dst_ref=c_all.at[index], send_sem=c_ss, recv_sem=c_rs,
            device_id=peer(k), device_id_type=pl.DeviceIdType.MESH,
        )

    for t in far_first:
        far_copy(t).start()
    near_copy(0).start()
    per_row = LANES // rank
    packed = rank // per_row
    sub = lax.broadcasted_iota(jnp.int32, (rank, LANES), 0)
    lane = lax.broadcasted_iota(jnp.int32, (rank, LANES), 1)
    own = lane // rank == lax.rem(sub, per_row)

    both = jnp.concatenate(split(mine), axis=0)
    core = lax.dot_general(both, both, NT, preferred_element_type=F32) / order
    core = core[:rank] + core[rank:]
    core = core[:, :rank] + core[:, rank:]
    wide = jnp.where(own, jnp.concatenate([core] * per_row, axis=1), 0.0)
    flat = jnp.concatenate(
        [jnp.sum(wide[a * per_row : (a + 1) * per_row, :], axis=0, keepdims=True) for a in range(packed)], axis=0
    )
    c_src[...] = flat
    c_all[index] = flat

    def send_core(k, carry):
        core_copy(k).start()
        return carry

    loop(1, devices, send_core)
    for t in reversed(far_first):
        far_copy(t).wait_recv()
        near_copy(t).start()
    all_received(img.at[pl.ds(0, half)], f_rs)
    for r in range(R):
        image_ref[:, r * part : (r + 1) * part] = img[r]
    all_received(c_all.at[pl.ds(0, devices - 1)], c_rs)
    flat = jnp.sum(c_all[...], axis=0)
    wide = jnp.concatenate(
        [jnp.broadcast_to(flat[a : a + 1, :], (per_row, LANES)) for a in range(packed)], axis=0
    )
    wide = jnp.where(own, wide, 0.0)
    shift = LANES // 2
    while shift >= rank:
        wide = wide + pltpu.roll(wide, shift, 1)
        shift //= 2
    core_ref[...] = wide[:, 0:rank]

    if C > 1:
        all_sent(sk_all.at[pl.ds(0, C - 1)], sk_ss)
    all_sent(g_all.at[pl.ds(0, R - 1)], g_ss)
    all_sent(s_in, p_ss)
    if half > 1:
        all_sent(w_all.at[pl.ds(0, half - 1)], w_ss)
        all_sent(img.at[pl.ds(0, half - 1)], a_ss)
    all_sent(img.at[pl.ds(0, half)], f_ss)
    all_sent(c_all.at[pl.ds(0, devices - 1)], c_ss)


def finish(*refs):
    copies = [pltpu.make_async_copy(refs[i], refs[3 + i], refs[6].at[i]) for i in range(3)]
    for copy in copies:
        copy.start()
    for copy in copies:
        copy.wait()


def shards(row_cells, col_cells, omega):
    R, C = lax.axis_size("row"), lax.axis_size("col")
    rank = omega.shape[0]
    M, N = row_cells.shape[1], col_cells.shape[1]
    chunk = min(M, UNIT)
    chunks, part, half = M // chunk, N // R, R // 2
    groups = chunks // max(chunks // 2, 1)
    shape = (R, C, rank, M, N, M * R, N * C)
    vmem = pltpu.VMEM
    dma = pltpu.SemaphoreType.DMA
    full = pl.BlockSpec(memory_space=pltpu.VMEM)
    hbm = pl.BlockSpec(memory_space=pltpu.HBM)
    out_shape = (
        jax.ShapeDtypeStruct((rank, M), F32),
        jax.ShapeDtypeStruct((rank, N), F32),
        jax.ShapeDtypeStruct((rank, rank), F32),
    )
    outs = pl.pallas_call(
        functools.partial(kernel, shape),
        out_shape=out_shape,
        in_specs=[hbm] * 3,
        out_specs=(full,) * 3,
        scratch_shapes=[
            vmem(row_cells.shape, jnp.int32),
            vmem(col_cells.shape, jnp.int32),
            vmem((rank, N), F32),
            vmem((16, M), BF16),
            vmem((N, LANES), BF16),
            vmem((2 * rank, N), BF16),
            vmem((N // LANES, M, LANES), BF16),
            vmem((N // LANES, M, LANES), BF16),
            *[vmem((UNIT, chunk), F32)] * BUFS,
            *[vmem((chunk // LANES, UNIT, LANES), BF16)] * 4,
            vmem((chunks, rank, chunk), F32),
            vmem((C, chunks, rank, chunk), F32),
            vmem((2 * rank, M), BF16),
            vmem((rank, LANES), F32),
            vmem((R, rank, LANES), F32),
            vmem((half, 2, rank, part), F32),
            vmem((half, 2, rank, part), F32),
            vmem((half, rank, part), F32),
            vmem((half, rank, part), F32),
            vmem((half, rank, part), F32),
            vmem((R, rank, part), F32),
            vmem((rank * rank // LANES, LANES), F32),
            vmem((R * C, rank * rank // LANES, LANES), F32),
            dma((3,)), dma((groups,)), dma((half,)), dma((half,)), dma((11,)),
        ],
        compiler_params=pltpu.CompilerParams(
            collective_id=0, has_side_effects=True, vmem_limit_bytes=VMEM_LIMIT,
        ),
    )(*(pltpu.with_memory_space_constraint(x, pltpu.HBM) for x in (row_cells, col_cells, omega)))
    return pl.pallas_call(
        finish,
        out_shape=out_shape,
        in_specs=[full] * 3,
        out_specs=(hbm,) * 3,
        scratch_shapes=[dma((3,))],
        compiler_params=pltpu.CompilerParams(vmem_limit_bytes=4 * 1024 * 1024),
    )(*outs)


def solution(mesh):
    return jax.shard_map(
        shards,
        mesh=mesh,
        in_specs=(P(None, "row"), P(None, "col"), P(None, "col")),
        out_specs=(P(None, "row"), P(None, "col"), P()),
        check_vma=False,
    )
```

```python
import functools
import math

import jax
import jax.numpy as jnp
from jax import lax
from jax.experimental import pallas as pl
from jax.experimental.pallas import tpu as pltpu
from jax.sharding import PartitionSpec as P

BF16, F32 = jnp.bfloat16, jnp.float32
HIGHEST = lax.Precision.HIGHEST
NT = (((1,), (1,)), ((), ()))
NN = (((1,), (0,)), ((), ()))
LANES = 128
RATE = -math.log2(math.e) / 6.4
UNIT = 256
LEAD = 4
BUFS = 8
SLICE = 64
VMEM_LIMIT = 48000 * 1024


def split(x):
    high = x.astype(BF16)
    return high, (x - high.astype(F32)).astype(BF16)


def loop(first, last, body):
    if last - first < 64:
        for k in range(first, last):
            body(k, 0)
    else:
        lax.fori_loop(first, last, body, 0)


def features(cells, left):
    x = [cells[d : d + 1, :].astype(F32) - 32.0 for d in range(3)]
    norm = x[0] * x[0] + x[1] * x[1] + x[2] * x[2]
    high = jnp.floor(norm * 0.0625) * 16.0
    low = norm - high
    one, zero = jnp.ones_like(norm), jnp.zeros_like(norm)
    if left:
        rows = [-2.0 * x[0], -2.0 * x[1], -2.0 * x[2], one, one, high, low, zero]
    else:
        rows = [x[0], x[1], x[2], high, low, one, one, zero]
    return jnp.concatenate(rows, axis=0)


def kernel(
    shape,
    row_hbm, col_hbm, omega_hbm,
    basis_ref, image_ref, core_ref,
    row_in, col_in, om_in, rowf, colf, om, khi, klo, sq0, sq1, sq2, sq3, sq4, sq5, sq6, sq7, hi0, hi1, lo0, lo1,
    sk_src, sk_all, sk_hl, g_src, g_all, wacc, wp, s_in, w_src, w_all, img, c_src, c_all,
    in_s, sk_rs, p_rs, a_rs, one_s,
):
    R, C, rank, M, N, rows_total, order = shape
    me = lax.axis_index("row")
    mc = lax.axis_index("col")
    half = R // 2
    side = lax.rem(me, 2)
    chip = me // 2
    sib = me + 1 - 2 * side
    part = N // R
    chunk = min(M, UNIT)
    chunks = M // chunk
    group = max(chunks // 2, 1)
    groups = chunks // group
    devices = R * C
    index = mc * R + me
    units = N // UNIT
    sq = (sq0, sq1, sq2, sq3, sq4, sq5, sq6, sq7)
    hi, lo = (hi0, hi1), (lo0, lo1)
    binary = half & (half - 1) == 0
    far_first = sorted(range(1, half), key=lambda t: -bin(t).count("1"))

    def row_of(t):
        return lax.rem(me + t, R)

    def chip_to(t):
        if not binary:
            return lax.rem(chip + t, half)
        total, bit = 0, 1
        while bit < half:
            total = total + bit * lax.rem(chip // bit + t // bit, 2)
            bit *= 2
        return total

    def chip_from(t):
        return chip_to(t) if binary else lax.rem(chip + half - t, half)

    def remote(src, dst, ss, rs, axis, peer):
        return pltpu.make_async_remote_copy(
            src_ref=src, dst_ref=dst, send_sem=ss, recv_sem=rs,
            device_id={axis: peer}, device_id_type=pl.DeviceIdType.MESH,
        )

    sk_ss, g_ss, g_rs, p_ss, w_ss, w_rs, a_ss, f_ss, f_rs, c_ss, c_rs = (one_s.at[i] for i in range(11))

    def all_sent(ref, ss):
        remote(ref, ref, ss, ss, "row", sib).wait_send()

    def all_received(ref, rs):
        remote(ref, ref, rs, rs, "row", sib).wait_recv()

    loads = [
        pltpu.make_async_copy(source, target, in_s.at[i])
        for i, (source, target) in enumerate(((omega_hbm, om_in), (col_hbm, col_in), (row_hbm, row_in)))
    ]
    for load in loads:
        load.start()
    barrier = pltpu.get_barrier_semaphore()

    def peer(k):
        other = lax.rem(index + k, devices)
        return {"row": lax.rem(other, R), "col": other // R}

    def greet(k, carry):
        pl.semaphore_signal(barrier, inc=1, device_id=peer(k), device_id_type=pl.DeviceIdType.MESH)
        return carry

    loop(1, devices, greet)

    loads[0].wait()
    loads[1].wait()
    loads[2].wait()
    rowf[0:8, :] = features(row_in[...], False).astype(BF16)
    rowf[8:16, :] = jnp.zeros((8, M), BF16)
    step = min(N, 1024)
    for s in range(N // step):
        left = features(col_in[:, s * step : (s + 1) * step], True)
        left = jnp.concatenate([left, jnp.zeros((8, step), F32)], axis=0).astype(BF16)
        for b in range(step // LANES):
            block = jnp.concatenate(
                [left[:, b * LANES : (b + 1) * LANES], jnp.zeros((LANES - 16, LANES), BF16)], axis=0
            )
            colf[s * step + b * LANES : s * step + (b + 1) * LANES, :] = block.T
    for s in range(N // step):
        cols = pl.ds(s * step, step)
        high, low = split(0.25 * om_in[:, cols])
        om[0:rank, cols] = high
        om[rank : 2 * rank, cols] = low

    def sketch_copy(rc, t):
        return remote(
            sk_src.at[rc], sk_all.at[mc, rc], sk_ss, sk_rs.at[rc // group], "col", lax.rem(mc + t, C)
        )

    def squared(u, right):
        return lax.dot_general(
            colf[u * UNIT : (u + 1) * UNIT, 0:16], right, NN, preferred_element_type=F32
        )

    for u in range(LEAD):
        sq[u][...] = squared(u, rowf[:, 0:chunk])

    def row_chunk(rc, carry):
        start = pl.multiple_of(rc * chunk, chunk)
        right = rowf[:, pl.ds(start, chunk)]
        right_next = rowf[:, pl.ds(pl.multiple_of(lax.rem(rc + 1, chunks) * chunk, chunk), chunk)]

        def use(u, acc):
            o = om[:, u * UNIT : (u + 1) * UNIT]
            for stage, whole in ((hi, khi), (lo, klo)):
                tile = jnp.concatenate([stage[u % 2][q] for q in range(chunk // LANES)], axis=1)
                acc = acc + lax.dot_general(o, tile, NN, preferred_element_type=F32)
                for q in range(chunk // LANES):
                    for p in range(UNIT // LANES):
                        whole[u * (UNIT // LANES) + p, pl.ds(start + q * LANES, LANES), :] = (
                            stage[u % 2][q, p * LANES : (p + 1) * LANES, :].T
                        )
            return acc

        acc = jnp.zeros((2 * rank, chunk), F32)
        for u in range(units):
            ahead = u + LEAD
            sq[ahead % BUFS][...] = squared(ahead % units, right if ahead < units else right_next)
            if u > 0:
                acc = use(u - 1, acc)
            for s in range(UNIT // SLICE):
                rows = slice(s * SLICE, (s + 1) * SLICE)
                value = jnp.maximum(sq[u % BUFS][rows, :], 1e-30)
                value = jnp.exp2((value * RATE) * lax.rsqrt(value))
                high, low = split(value)
                for q in range(chunk // LANES):
                    hi[u % 2][q, rows, :] = high[:, q * LANES : (q + 1) * LANES]
                    lo[u % 2][q, rows, :] = low[:, q * LANES : (q + 1) * LANES]
        acc = use(units - 1, acc)
        total = acc[:rank] + acc[rank:]

        @pl.when(rc == 0)
        def _():
            pl.semaphore_wait(barrier, devices - 1)

        sk_src[rc] = total
        sk_all[mc, rc] = total
        for t in range(1, C):
            sketch_copy(rc, t).start()
        return carry

    lax.fori_loop(0, chunks, row_chunk, 0)

    tiles = 2 * part // LANES

    def product(base, g, count):
        rows = slice(g * group * chunk, (g + 1) * group * chunk)
        s = sk_hl[:, rows]
        acc = None
        for whole in (khi, klo):
            block = jnp.concatenate([whole[base + i, rows, :] for i in range(count)], axis=1)
            term = lax.dot_general(s, block, NN, preferred_element_type=F32)
            acc = term if acc is None else acc + term
        return acc[:rank] + acc[rank:]

    def take(g):
        if C > 1:
            all_received(sk_all.at[pl.ds(0, C - 1), pl.ds(0, group)], sk_rs.at[g])
        pieces = []
        for rc in range(g * group, (g + 1) * group):
            total = sk_all[0, rc]
            for c in range(1, C):
                total = total + sk_all[c, rc]
            pieces.append(total)
        sketch = jnp.concatenate(pieces, axis=1)
        high, low = split(0.25 * sketch)
        rows = slice(g * group * chunk, (g + 1) * group * chunk)
        sk_hl[0:rank, rows] = high
        sk_hl[rank : 2 * rank, rows] = low
        return sketch, lax.dot_general(sketch, sketch, NT, precision=HIGHEST, preferred_element_type=F32)

    def early(t, g):
        to = chip_to(t)
        acc = product(to * tiles, g, tiles)
        for which in range(2):
            some = acc[:, which * part : (which + 1) * part]
            wacc[to, which] = some if g == 0 else some + wacc[to, which]

    parts, gram = [], None
    for g in range(groups):
        some, term = take(g)
        parts.append(some)
        gram = term if gram is None else gram + term
        if g == groups - 1:
            break

        for t in far_first:
            early(t, g)
    sketch = jnp.concatenate(parts, axis=1)
    g_src[...] = jnp.zeros_like(g_src)
    g_src[:, rank : 2 * rank] = gram / rows_total
    g_all[me] = g_src[...]

    def gram_copy(t):
        return remote(g_src, g_all.at[me], g_ss, g_rs, "row", row_of(t))

    for t in range(1, R):
        gram_copy(t).start()

    def pair_copy(t):
        return remote(wp.at[t, 1 - side], s_in.at[t], p_ss, p_rs.at[t], "row", sib)

    def w_copy(t):
        return remote(w_src.at[t], w_all.at[t], w_ss, w_rs, "row", 2 * chip_to(t) + side)

    def blocks(t):
        to = chip_to(t)
        for which in (1 - side, side):
            acc = product(to * tiles + which * (tiles // 2), groups - 1, tiles // 2)
            if groups > 1:
                acc = acc + wacc[to, which]
            wp[t, which] = acc
            if which is not side:
                pair_copy(t).start()

    def forward(t):
        pair_copy(t).wait_recv()
        w_src[t] = wp[t, side] + s_in[t]
        w_copy(t).start()

    before = None
    for t in far_first:
        blocks(t)
        if before is not None:
            forward(before)
        before = t
    for g in range(groups - 1):
        early(0, g)
    if before is not None:
        forward(before)
    all_received(g_all.at[pl.ds(0, R - 1)], g_rs)
    blocks(0)
    mat = g_all[0]
    for r in range(1, R):
        mat = mat + g_all[r]
    sub = lax.broadcasted_iota(jnp.int32, mat.shape, 0)
    lane = lax.broadcasted_iota(jnp.int32, mat.shape, 1)
    mat = mat + jnp.where(lane == sub, 1.0, 0.0)
    for k in range(rank - 1):
        row = mat[k : k + 1, :]
        factor = mat[:, rank + k : rank + k + 1] * (1.0 / mat[k : k + 1, rank + k : rank + k + 1])
        mat = mat - jnp.where(sub > k, factor * row, 0.0)
    diag = jnp.sum(jnp.where(lane == sub + rank, mat, 0.0), axis=1, keepdims=True)
    inverse = (mat * (1.0 / jnp.sqrt(diag)))[:, :rank]
    inverse = jnp.where(lane[:, :rank] <= sub[:, :rank], inverse, 0.0)
    basis_ref[...] = jnp.dot(inverse, sketch, precision=HIGHEST, preferred_element_type=F32)
    pair_copy(0).wait_recv()
    total = wp[0, side] + s_in[0]
    if half > 1:
        all_received(w_all.at[pl.ds(0, half - 1)], w_rs)
    for t in far_first:
        total = total + w_all[t]
    mine = jnp.dot(inverse, total, precision=HIGHEST, preferred_element_type=F32)
    img[me] = mine

    def far_copy(t):
        return remote(img.at[me], img.at[me], a_ss, a_rs.at[t], "row", 2 * chip_to(t) + side)

    def near_copy(t):
        slot = 2 * chip_from(t) + side
        return remote(img.at[slot], img.at[slot], f_ss, f_rs, "row", sib)

    def core_copy(k):
        return pltpu.make_async_remote_copy(
            src_ref=c_src, dst_ref=c_all.at[index], send_sem=c_ss, recv_sem=c_rs,
            device_id=peer(k), device_id_type=pl.DeviceIdType.MESH,
        )

    for t in far_first:
        far_copy(t).start()
    near_copy(0).start()
    per_row = LANES // rank
    packed = rank // per_row
    sub = lax.broadcasted_iota(jnp.int32, (rank, LANES), 0)
    lane = lax.broadcasted_iota(jnp.int32, (rank, LANES), 1)
    own = lane // rank == lax.rem(sub, per_row)

    both = jnp.concatenate(split(mine), axis=0)
    core = lax.dot_general(both, both, NT, preferred_element_type=F32) / order
    core = core[:rank] + core[rank:]
    core = core[:, :rank] + core[:, rank:]
    wide = jnp.where(own, jnp.concatenate([core] * per_row, axis=1), 0.0)
    flat = jnp.concatenate(
        [jnp.sum(wide[a * per_row : (a + 1) * per_row, :], axis=0, keepdims=True) for a in range(packed)], axis=0
    )
    c_src[...] = flat
    c_all[index] = flat

    def send_core(k, carry):
        core_copy(k).start()
        return carry

    loop(1, devices, send_core)
    for t in reversed(far_first):
        far_copy(t).wait_recv()
        near_copy(t).start()
    all_received(img.at[pl.ds(0, half)], f_rs)
    for r in range(R):
        image_ref[:, r * part : (r + 1) * part] = img[r]
    all_received(c_all.at[pl.ds(0, devices - 1)], c_rs)
    flat = jnp.sum(c_all[...], axis=0)
    wide = jnp.concatenate(
        [jnp.broadcast_to(flat[a : a + 1, :], (per_row, LANES)) for a in range(packed)], axis=0
    )
    wide = jnp.where(own, wide, 0.0)
    shift = LANES // 2
    while shift >= rank:
        wide = wide + pltpu.roll(wide, shift, 1)
        shift //= 2
    core_ref[...] = wide[:, 0:rank]

    if C > 1:
        all_sent(sk_all.at[pl.ds(0, C - 1)], sk_ss)
    all_sent(g_all.at[pl.ds(0, R - 1)], g_ss)
    all_sent(s_in, p_ss)
    if half > 1:
        all_sent(w_all.at[pl.ds(0, half - 1)], w_ss)
        all_sent(img.at[pl.ds(0, half - 1)], a_ss)
    all_sent(img.at[pl.ds(0, half)], f_ss)
    all_sent(c_all.at[pl.ds(0, devices - 1)], c_ss)


def finish(*refs):
    copies = [pltpu.make_async_copy(refs[i], refs[3 + i], refs[6].at[i]) for i in range(3)]
    for copy in copies:
        copy.start()
    for copy in copies:
        copy.wait()


def shards(row_cells, col_cells, omega):
    R, C = lax.axis_size("row"), lax.axis_size("col")
    rank = omega.shape[0]
    M, N = row_cells.shape[1], col_cells.shape[1]
    chunk = min(M, UNIT)
    chunks, part, half = M // chunk, N // R, R // 2
    groups = chunks // max(chunks // 2, 1)
    shape = (R, C, rank, M, N, M * R, N * C)
    vmem = pltpu.VMEM
    dma = pltpu.SemaphoreType.DMA
    full = pl.BlockSpec(memory_space=pltpu.VMEM)
    hbm = pl.BlockSpec(memory_space=pltpu.HBM)
    out_shape = (
        jax.ShapeDtypeStruct((rank, M), F32),
        jax.ShapeDtypeStruct((rank, N), F32),
        jax.ShapeDtypeStruct((rank, rank), F32),
    )
    outs = pl.pallas_call(
        functools.partial(kernel, shape),
        out_shape=out_shape,
        in_specs=[hbm] * 3,
        out_specs=(full,) * 3,
        scratch_shapes=[
            vmem(row_cells.shape, jnp.int32),
            vmem(col_cells.shape, jnp.int32),
            vmem((rank, N), F32),
            vmem((16, M), BF16),
            vmem((N, LANES), BF16),
            vmem((2 * rank, N), BF16),
            vmem((N // LANES, M, LANES), BF16),
            vmem((N // LANES, M, LANES), BF16),
            *[vmem((UNIT, chunk), F32)] * BUFS,
            *[vmem((chunk // LANES, UNIT, LANES), BF16)] * 4,
            vmem((chunks, rank, chunk), F32),
            vmem((C, chunks, rank, chunk), F32),
            vmem((2 * rank, M), BF16),
            vmem((rank, LANES), F32),
            vmem((R, rank, LANES), F32),
            vmem((half, 2, rank, part), F32),
            vmem((half, 2, rank, part), F32),
            vmem((half, rank, part), F32),
            vmem((half, rank, part), F32),
            vmem((half, rank, part), F32),
            vmem((R, rank, part), F32),
            vmem((rank * rank // LANES, LANES), F32),
            vmem((R * C, rank * rank // LANES, LANES), F32),
            dma((3,)), dma((groups,)), dma((half,)), dma((half,)), dma((11,)),
        ],
        compiler_params=pltpu.CompilerParams(
            collective_id=0, has_side_effects=True, vmem_limit_bytes=VMEM_LIMIT,
        ),
    )(*(pltpu.with_memory_space_constraint(x, pltpu.HBM) for x in (row_cells, col_cells, omega)))
    return pl.pallas_call(
        finish,
        out_shape=out_shape,
        in_specs=[full] * 3,
        out_specs=(hbm,) * 3,
        scratch_shapes=[dma((3,))],
        compiler_params=pltpu.CompilerParams(vmem_limit_bytes=4 * 1024 * 1024),
    )(*outs)


def solution(mesh):
    return jax.shard_map(
        shards,
        mesh=mesh,
        in_specs=(P(None, "row"), P(None, "col"), P(None, "col")),
        out_specs=(P(None, "row"), P(None, "col"), P()),
        check_vma=False,
    )
```
